32 devices in a mesh: rep: 4 (over z), ep: 8 (over y, x, core).
Axes of the slice: x: 2, y: 2, z: 4, core: 2. Of those that a mesh axis runs over, the one named last changes fastest.
Arguments:
- latent_pages: bfloat16 [1536, 36864], P(('rep', 'ep')), may hold values from -4 to 4
- queries: bfloat16 [256, 147456], P(('rep', 'ep')), may hold values from -4 to 4
- residual: bfloat16 [256, 14336], P(('rep', 'ep')), may hold values from -6 to 6
- page_count: int32 [4, 8, 8], P(None, 'ep'), may hold values from 1 to 12, 48 in all within a row
- last_fill: int32 [4, 8, 8], P(None, 'ep'), may hold values from 4 to 64
- page_order: int32 [32, 48], P(('rep', 'ep')), may hold values from 0 to 47, each once within a row
- shed_slots: int32 [4, 8, 2], P(None, 'ep'), may hold values from 0 to 7, as said below
- shed_shift: int32 [8, 2], P('ep'), may hold values from 1 to 3
- expert_ids: int32 [1024, 8], P(('rep', 'ep')), may hold values from 0 to 31, all different within a row; in each aligned block of 32 rows (0 to 31, 32 to 63, ...) at most 16 rows name the same one
- gate_weight: float32 [1024, 8], P(('rep', 'ep')), may hold values from 0.05 to 0.5
- expert_home: int32 [32], replicated, may hold values from 0 to 31, each once
- norm_gain: float32 [3584], replicated, may hold values from 0.1 to 1.9
- value_up: bfloat16 [64, 512, 128], P('ep'), may hold values from -0.59765625 to 0.59765625
- out_weight: bfloat16 [8192, 3584], P('ep'), may hold values from -0.14941406 to 0.14941406
- expert_in: bfloat16 [32, 3584, 1024], P(('rep', 'ep')), may hold values from -0.09375 to 0.09375
- expert_out: bfloat16 [32, 1024, 3584], P(('rep', 'ep')), may hold values from -0.1875 to 0.1875
Outputs:
- attn_proj: bfloat16 [256, 14336], P(('rep', 'ep'))
- layer_out: bfloat16 [256, 14336], P(('rep', 'ep'))
The draws below stay inside these ranges and needn't reach their ends.
Inputs may be any that keep to these rules, and one draw needn't show every extreme that they name: `shed_slots`: for each device, 2 different slots. `expert_ids`: each row names 8 different experts; in the rows of one device no expert is named by more than 16 rows.
All inputs are finite; a program needn't handle non-finite values.
Results may differ from the reference program's by a relative error of at most 0.015.
Values may be sent and summed in bfloat16 or wider, within the bound.
A program may use at most 192 MiB of HBM per device.

```python
import math
import jax
import jax.numpy as jnp
import numpy as np
from jax import lax

D = 3584
HEADS = 64
LAT = 512
KVW = 576
VHEAD = 128
FFE = 1024
TOP = 8
PAGE = 64
SPEC = 4
MAXP = 12
REQ_DEV = 8
SHED = 2
PAGES_DEV = 48
REQUESTS = 256
TOK_DEV = 32
TOKENS = 1024
EXPERTS = 32
CAP = 16
N_REP = 4
N_EP = 8
DEVICES = 32


def draw_latent_pages(key, part):
    page_shape = (N_REP * N_EP * PAGES_DEV, PAGE, KVW)
    values = jnp.clip(jax.random.normal(key, page_shape, jnp.float32), -4.0, 4.0)
    return values.reshape(N_REP * N_EP * PAGES_DEV, PAGE * KVW).astype(jnp.bfloat16)


def draw_queries(key, part):
    ask_shape = (N_REP * N_EP * REQ_DEV, SPEC * HEADS, KVW)
    values = jnp.clip(jax.random.normal(key, ask_shape, jnp.float32), -4.0, 4.0)
    return values.reshape(N_REP * N_EP * REQ_DEV, SPEC * HEADS * KVW).astype(jnp.bfloat16)


def draw_shed_slots(key, part):
    split_keys = jax.random.split(jax.random.fold_in(key, 11), N_REP * N_EP)
    orders = jax.vmap(lambda single_key: jax.random.permutation(single_key, REQ_DEV))(split_keys)
    return orders[:, :SHED].reshape(N_REP, N_EP, SHED).astype(jnp.int32)


def with_ends(values, stream_key, least, largest):
    index_at = [jax.random.randint(jax.random.fold_in(stream_key, axis), (), 0, length) for axis, length in enumerate(values.shape)]
    longest = values.shape.index(max(values.shape))
    neighbour = index_at[:longest] + [(index_at[longest] + 1) % values.shape[longest]] + index_at[longest + 1:]
    return values.at[tuple(index_at)].set(least).at[tuple(neighbour)].set(largest)


def block_scale(stream_key, extent, pieces, least, largest):
    gain = 1.0
    for axis_at, parts in pieces:
        steps = jax.random.uniform(jax.random.fold_in(jax.random.fold_in(stream_key, 6), axis_at), (parts,), jnp.float32, least / len(pieces), largest / len(pieces))
        gain = gain * jnp.repeat(jnp.exp(steps), extent[axis_at] // parts).reshape((-1,) + (1,) * (len(extent) - 1 - axis_at))
    return gain


def profile(number_of, total, most, skew):
    portions = [(1 << 20) // math.isqrt(standing ** skew) + 1 for standing in range(2, number_of + 1)]
    spare, holding = total - most - (number_of - 1), [1] * (number_of - 1)
    while spare > 0:
        free = [i for i in range(number_of - 1) if holding[i] < most]
        whole, remaining = sum([portions[i] for i in free]), spare
        for i in free:
            more = min(most - holding[i], max(1, remaining * portions[i] // whole), spare)
            holding[i] = holding[i] + more
            spare = spare - more
    return np.array([most] + holding)


def uneven(stream_key, number_of, total, limit, lean):
    if number_of == 2:
        one = jax.random.randint(stream_key, (), max(1, total - limit), min(limit, total - 1) + 1)
        return jnp.stack([one, total - one])
    sizes = jnp.asarray(profile(number_of, total, limit, lean), jnp.int32)
    couples = (number_of - 1) // 2
    donor, sink = sizes[1:1 + 2 * couples:2], sizes[2:2 + 2 * couples:2]
    margin = jnp.minimum(donor - 1, limit - sink)
    moved = jax.random.randint(jax.random.fold_in(stream_key, 1), (couples,), 0, 1 << 20) % (margin + 1)
    sizes = sizes.at[1:1 + 2 * couples:2].set(donor - moved).at[2:2 + 2 * couples:2].set(sink + moved)
    return sizes[jax.random.permutation(jax.random.fold_in(stream_key, 2), number_of)]


def routed_block(key, own, number, rows, count, top, limit, skew):
    order = jax.random.permutation(key, count)
    heavy_load, usual = shares(count, rows * top, limit, skew, True), shares(count, rows * top, limit, skew, False)
    places = jnp.arange(count)

    def named(tallies, turn):
        used = int((tallies > 0).sum())
        fixed = max(1, used // 4)
        passed = fixed + (places - fixed + turn * (used - fixed)) % max(1, count - fixed)
        return jnp.zeros((count,), jnp.int32).at[order[jnp.where(places < fixed, places, passed)]].set(jnp.asarray(tallies, jnp.int32))

    tallies = jnp.where(number % 4 == 0, named(heavy_load, number // 4), named(usual, number - number // 4 - 1))
    mixed = jax.random.permutation(jax.random.fold_in(own, 3), count)
    source_of, receiver = mixed[0:count // 2 * 2:2], mixed[1:count // 2 * 2:2]
    slack = jnp.minimum(tallies[source_of] - 1, limit - tallies[receiver]) // 2
    slack = jnp.where((source_of == order[0]) | (receiver == order[0]) | (tallies[receiver] == 0), 0, jnp.maximum(slack, 0))
    passed = jax.random.randint(jax.random.fold_in(own, 4), (count // 2,), 0, 1 << 20) % (slack + 1)
    tallies = tallies.at[source_of].add(-passed).at[receiver].add(passed)
    items = jnp.searchsorted(jnp.cumsum(tallies), jnp.arange(rows * top), side="right").astype(jnp.int32)
    grid = items.reshape(top, rows).T
    grid = grid[jax.random.permutation(jax.random.fold_in(own, 1), rows)]
    turn = jax.random.randint(jax.random.fold_in(own, 2), (rows, 1), 0, top)
    return jnp.take_along_axis(grid, (jnp.arange(top)[None, :] + turn) % top, axis=1)


def shares(count, total, reach, skew, full):
    loads = [(1 << 20) // math.isqrt(standing ** skew) + 1 for standing in range(1, count + 1)]
    largest = reach if full else min(reach, max(-(-total // count), total * loads[0] // sum(loads)))
    least = 1 if total - largest >= count - 1 else 0
    holding, spare = [largest] + [least] * (count - 1), total - largest - least * (count - 1)
    while spare > 0:
        free = [i for i in range(1, count) if holding[i] < largest] or [i for i in range(1, count) if holding[i] < reach]
        pool, remaining = sum([loads[i] for i in free]), spare
        for i in free:
            extra = min(reach - holding[i], max(1, remaining * loads[i] // pool), spare)
            holding[i] = holding[i] + extra
            spare = spare - extra
    return np.array(holding)


def normal_values(key, extent, width, bound, shards=(), held_as=jnp.bfloat16):
    array = width * jax.random.normal(key, extent, jnp.float32)
    if shards:
        array = array * block_scale(key, extent, shards, -0.22, 0.18)
    return jnp.clip(array, -bound, bound).astype(held_as)


def setup_inputs(seed: int = 0) -> dict:
    splits = jax.random.split(jax.random.key(seed), 17)
    latent_pages = draw_latent_pages(jax.random.fold_in(splits[16], 71), 0)
    queries = draw_queries(jax.random.fold_in(splits[16], 71), 0)
    residual = normal_values(splits[2], (REQUESTS, SPEC * D), 1.0, 6.0, ((0, 32),))
    page_count = jax.vmap(lambda own: uneven(own, REQ_DEV, PAGES_DEV, MAXP, 2))(jax.random.split(splits[3], N_REP * N_EP)).reshape((N_REP, N_EP, REQ_DEV)).astype(jnp.int32)
    last_fill = with_ends(jax.random.randint(splits[4], (N_REP, N_EP, REQ_DEV), SPEC, PAGE + 1), jax.random.fold_in(splits[4], 1), SPEC, PAGE).astype(jnp.int32)
    page_order = jax.vmap(lambda own: jax.random.permutation(own, PAGES_DEV))(jax.random.split(splits[5], DEVICES)).reshape((DEVICES, PAGES_DEV)).astype(jnp.int32)
    shed_slots = draw_shed_slots(jax.random.fold_in(splits[16], 71), 0)
    shed_shift = with_ends(jax.random.randint(splits[7], (N_EP, SHED), 1, N_REP), jax.random.fold_in(splits[7], 1), 1, N_REP - 1).astype(jnp.int32)
    expert_ids_keys = jax.random.split(jax.random.fold_in(splits[8], 1), TOKENS // TOK_DEV)
    expert_ids_turns = jax.random.permutation(jax.random.fold_in(splits[8], 3), TOKENS // TOK_DEV)
    expert_ids = jax.vmap(lambda own, number: routed_block(jax.random.fold_in(splits[8], 2), own, number, TOK_DEV, EXPERTS, TOP, CAP, 2))(expert_ids_keys, expert_ids_turns).reshape((TOKENS, TOP))
    gate_weight = jnp.clip(0.05 + 0.45 * jax.random.uniform(splits[9], (TOKENS, TOP), jnp.float32) ** block_scale(splits[9], (TOKENS, TOP), ((0, 32),), -0.2, 0.2), 0.05, 0.5)
    expert_home = jax.random.permutation(splits[10], EXPERTS).astype(jnp.int32)
    norm_gain = jnp.clip(1.0 + 0.18 * jax.random.normal(splits[11], (D,), jnp.float32), 0.1, 1.9)
    value_up = normal_values(splits[12], (HEADS, LAT, VHEAD), 0.1, 0.59765625, ((0, 8),))
    out_weight = normal_values(splits[13], (HEADS * VHEAD, D), 0.025, 0.14941406, ((0, 8),))
    expert_in = normal_values(splits[14], (EXPERTS, D, FFE), D ** -0.5, 0.09375, ((0, 32),))
    expert_out = normal_values(splits[15], (EXPERTS, FFE, D), FFE ** -0.5, 0.1875, ((0, 32),))
    return dict(latent_pages=latent_pages, queries=queries, residual=residual, page_count=page_count, last_fill=last_fill, page_order=page_order, shed_slots=shed_slots, shed_shift=shed_shift, expert_ids=expert_ids, gate_weight=gate_weight, expert_home=expert_home, norm_gain=norm_gain, value_up=value_up, out_weight=out_weight, expert_in=expert_in, expert_out=expert_out)


SCORE_SCALE = 192.0 ** (-0.5)
NORM_EPS = 0.25

def serve_source(shed_slots, shed_shift):
    replicas = jnp.arange(N_REP, dtype=jnp.int32)[:, None, None]
    columns = jnp.arange(N_EP, dtype=jnp.int32)[None, :, None]
    shed_rank = jnp.arange(SHED, dtype=jnp.int32)[None, None, :]
    anchor_rep = ((replicas - shed_shift[None, :, :]) % N_REP).astype(jnp.int32)
    anchor_slot = shed_slots[anchor_rep, columns, shed_rank]
    anchor_id = ((anchor_rep * N_EP + columns) * REQ_DEV + anchor_slot).astype(jnp.int32)
    target_id = ((replicas * N_EP + columns) * REQ_DEV + shed_slots).astype(jnp.int32)
    identity = jnp.arange(N_REP * N_EP * REQ_DEV, dtype=jnp.int32)
    return identity.at[target_id.reshape(-1)].set(anchor_id.reshape(-1))

def page_tables(page_count, page_order):
    counts_flat = page_count.reshape(N_REP * N_EP, REQ_DEV).astype(jnp.int32)
    offsets = (jnp.cumsum(counts_flat, axis=1) - counts_flat).astype(jnp.int32)
    page_steps = jnp.arange(MAXP, dtype=jnp.int32)
    positions = jnp.minimum(offsets[:, :, None] + page_steps[None, None, :], PAGES_DEV - 1).astype(jnp.int32)
    local_rows = jax.vmap(lambda order_row, spot_list: order_row[spot_list])(page_order, positions)
    base_rows = (jnp.arange(N_REP * N_EP, dtype=jnp.int32) * PAGES_DEV)[:, None, None]
    return (local_rows + base_rows).reshape(N_REP * N_EP * REQ_DEV, MAXP).astype(jnp.int32)

def attend_rows(key_rows, query_rows, length):
    scores = jnp.dot(query_rows, key_rows.T, preferred_element_type=jnp.float32) * SCORE_SCALE
    position = jnp.arange(MAXP * PAGE, dtype=jnp.int32)
    offset = jnp.arange(SPEC * HEADS, dtype=jnp.int32) // HEADS
    visible_end = length - SPEC + 1 + offset
    visible = position[None, :] < visible_end[:, None]
    scores = jnp.where(visible, scores, -1e+30)
    exponent = jnp.exp(scores - lax.optimization_barrier(jnp.max(scores, axis=1, keepdims=True)))
    probability = (exponent / lax.optimization_barrier(jnp.sum(exponent, axis=1, keepdims=True))).astype(jnp.bfloat16)
    return jnp.dot(probability, key_rows[:, :LAT], preferred_element_type=jnp.float32).astype(jnp.bfloat16)

def reference(latent_pages, queries, residual, page_count, last_fill, page_order, shed_slots, shed_shift, expert_ids, gate_weight, expert_home, norm_gain, value_up, out_weight, expert_in, expert_out):
    requests = N_REP * N_EP * REQ_DEV
    tokens = requests * SPEC
    source = serve_source(shed_slots, shed_shift)
    tables = page_tables(page_count, page_order)
    lengths = ((page_count - 1) * PAGE + last_fill).reshape(requests).astype(jnp.int32)

    def attend_slot(serving):
        anchor = source[serving]
        key_rows = latent_pages[tables[anchor]].reshape(MAXP * PAGE, KVW)
        query_rows = queries[anchor].reshape(SPEC * HEADS, KVW)
        return attend_rows(key_rows, query_rows, lengths[anchor])
    latent_out = lax.map(attend_slot, jnp.arange(requests, dtype=jnp.int32))
    replica_blocks = latent_out.reshape(N_REP, N_EP * REQ_DEV * SPEC, HEADS, LAT)

    def project(replica_rows):
        lifted = jnp.einsum('thl,hlv->thv', replica_rows.astype(jnp.float32), value_up.astype(jnp.float32)).astype(jnp.bfloat16)
        return jnp.dot(lifted.reshape(replica_rows.shape[0], HEADS * VHEAD), out_weight, preferred_element_type=jnp.float32)
    branch = lax.map(project, replica_blocks).reshape(tokens, D)
    mixed = residual[source].reshape(tokens, D).astype(jnp.float32) + branch
    square = lax.optimization_barrier(jnp.mean(mixed * mixed, axis=1, keepdims=True))
    normed = (mixed * lax.rsqrt(square + NORM_EPS) * norm_gain).astype(jnp.bfloat16)
    flat_ids = expert_ids.reshape(-1)
    flat_gates = gate_weight.reshape(-1)
    most_rows = N_REP * N_EP * CAP

    def expert_step(running, expert):
        chosen = flat_ids == expert
        found_at = jnp.nonzero(chosen, size=most_rows, fill_value=0)[0].astype(jnp.int32)
        filled = jnp.arange(most_rows) < jnp.sum(chosen)
        owners = (found_at // TOP).astype(jnp.int32)
        weights = jnp.where(filled, flat_gates[found_at], 0.0)
        placed = expert_home[expert]
        inner_act = jax.nn.silu(jnp.dot(normed[owners], expert_in[placed], preferred_element_type=jnp.float32)).astype(jnp.bfloat16)
        outer_out = jnp.dot(inner_act, expert_out[placed], preferred_element_type=jnp.float32).astype(jnp.bfloat16)
        return (running.at[owners].add(weights[:, None] * outer_out.astype(running.dtype)), None)
    moe_sum, unused = lax.scan(expert_step, jnp.zeros((tokens, D), jnp.float32), jnp.arange(EXPERTS, dtype=jnp.int32))
    attn_proj = branch.astype(jnp.bfloat16).reshape(requests, SPEC * D)
    layer_out = (mixed + moe_sum).astype(jnp.bfloat16).reshape(requests, SPEC * D)
    return (attn_proj, layer_out)
```

```python
import functools

import jax
import jax.numpy as jnp
from jax import lax
from jax.experimental import pallas as pl
from jax.experimental.pallas import tpu as pltpu
from jax.sharding import PartitionSpec as P

D = 3584
HEADS = 64
LAT = 512
KVW = 576
VHEAD = 128
TOP = 8
PAGE = 64
SPEC = 4
MAXP = 12
REQ_DEV = 8
PAGES_DEV = 48


SCORE_SCALE = 192.0 ** (-0.5)
NORM_EPS = 0.25
MESH = pl.DeviceIdType.MESH


def shifted(value, axis, steps):
    count = lax.axis_size(axis)
    pairs = [(source, (source + steps) % count) for source in range(count)]
    return lax.ppermute(value, axis, pairs)


def flipped(index, bit):
    width = 1 << bit
    return index + width * (1 - 2 * ((index // width) % 2))


def masked(index, mask):
    for bit in range(mask.bit_length()):
        if mask >> bit & 1:
            index = flipped(index, bit)
    return index


def submasks(bits):
    masks = [0]
    for bit in bits:
        masks = masks + [mask | 1 << bit for mask in masks]
    return masks


def greet(rep_count, bit_count, replica, column):
    barrier = pltpu.get_barrier_semaphore()
    for steps in range(1, rep_count):
        pl.semaphore_signal(barrier, inc=1, device_id=(lax.rem(replica + steps, rep_count), column), device_id_type=MESH)
    for bit in range(bit_count):
        pl.semaphore_signal(barrier, inc=1, device_id=(replica, flipped(column, bit)), device_id_type=MESH)
    pl.semaphore_wait(barrier, rep_count - 1 + bit_count)


def gather_plan(rep_count, bit_count):
    outer = list(range(1, bit_count))
    orders = (outer, outer[::-1])
    names = [("rep", steps) for steps in range(1, rep_count)]
    for half in range(2):
        for stage in range(len(outer)):
            for steps in range(rep_count):
                names += [(half, stage, steps, mask) for mask in submasks(orders[half][:stage])]
        for steps in range(rep_count):
            names += [("core", half, steps, mask) for mask in submasks(outer)]
    return orders, {name: at for at, name in enumerate(names)}


def gather_kernel(rep_count, col_count, in_ref, out_ref, send_sem, recv_sem, local_sem):
    bit_count = col_count.bit_length() - 1
    replica, column = lax.axis_index("rep"), lax.axis_index("ep")
    orders, number = gather_plan(rep_count, bit_count)
    half_rows = in_ref.shape[0] // 2
    greet(rep_count, bit_count, replica, column)

    def block(steps, mask, half):
        rows = slice(None) if half is None else pl.ds(half * half_rows, half_rows)
        origin = lax.rem(replica + rep_count - steps, rep_count)
        return out_ref.at[origin * col_count + masked(column, mask), rows]

    own = replica * col_count + column
    copies = {}

    def send(name, source, target, device):
        at = number[name]
        copies[name] = pltpu.make_async_remote_copy(
            src_ref=source, dst_ref=target, send_sem=send_sem.at[at], recv_sem=recv_sem.at[at],
            device_id=device, device_id_type=MESH,
        )
        copies[name].start()

    def spread(steps, half, mask, done):
        rows = pl.ds(half * half_rows, half_rows)
        source = in_ref.at[rows] if steps == 0 and mask == 0 else block(steps, mask, half)
        for stage in range(done, len(orders[half])):
            send((half, stage, steps, mask), source, block(steps, mask, half), (replica, flipped(column, orders[half][stage])))
        send(("core", half, steps, mask), source, block(steps, mask, half), (replica, flipped(column, 0)))

    for steps in range(1, rep_count):
        send(("rep", steps), in_ref, out_ref.at[own], (lax.rem(replica + steps, rep_count), column))
    for half in range(2):
        spread(0, half, 0, 0)
    mine = pltpu.make_async_copy(in_ref, out_ref.at[own], local_sem)
    mine.start()

    def arrivals(stage, steps):
        for half in range(2):
            bit = orders[half][stage]
            for mask in submasks(orders[half][:stage]):
                copies[(half, stage, steps, mask)].wait_recv()
                spread(steps, half, mask | 1 << bit, stage + 1)

    stages = len(orders[0])
    for turn in range(rep_count + stages):
        if 0 < turn < rep_count:
            copies[("rep", turn)].wait_recv()
            for half in range(2):
                spread(turn, half, 0, 0)
        for stage in range(stages):
            if 0 <= turn - stage < rep_count:
                arrivals(stage, turn - stage)
    mine.wait()
    for name, copy in copies.items():
        if name[0] == "core":
            copy.wait_recv()
        copy.wait_send()


def gather_all(rows, rep_count, col_count, collective_id):
    _, number = gather_plan(rep_count, col_count.bit_length() - 1)
    blocks = rep_count * col_count
    size = rows.size * 2
    out = pl.pallas_call(
        functools.partial(gather_kernel, rep_count, col_count),
        out_shape=jax.ShapeDtypeStruct((blocks,) + rows.shape, rows.dtype),
        in_specs=[pl.BlockSpec(memory_space=pltpu.VMEM)],
        out_specs=pl.BlockSpec(memory_space=pltpu.VMEM),
        scratch_shapes=[
            pltpu.SemaphoreType.DMA((len(number),)),
            pltpu.SemaphoreType.DMA((len(number),)),
            pltpu.SemaphoreType.DMA,
        ],
        compiler_params=pltpu.CompilerParams(
            collective_id=collective_id, has_side_effects=True, vmem_limit_bytes=size * (blocks + 2) + (2 << 20)
        ),
    )(rows)
    return out.reshape(blocks * rows.shape[0], rows.shape[1])


def scatter_plan(rep_count, bit_count):
    outer = list(range(1, bit_count))
    orders = (outer[::-1], outer)
    shifts = list(range(1, rep_count)) + [0]
    masks = sorted(submasks(outer), key=lambda mask: -bin(mask).count("1"))
    names = [("core", steps, mask) for steps in shifts for mask in masks]
    for half in range(2):
        for stage in range(len(outer)):
            for steps in shifts:
                names += [(half, stage, steps, mask) for mask in submasks(orders[half][stage + 1 :])]
        names += [("rep", half, steps) for steps in range(1, rep_count)]
    return orders, shifts, masks, {name: at for at, name in enumerate(names)}


def scatter_kernel(rep_count, col_count, in_ref, out_ref, core_buf, *rest):
    bit_count = col_count.bit_length() - 1
    stages = bit_count - 1
    stage_bufs, (rep_buf, send_sem, recv_sem) = rest[:stages], rest[stages:]
    replica, column = lax.axis_index("rep"), lax.axis_index("ep")
    orders, shifts, masks, number = scatter_plan(rep_count, bit_count)
    half_rows = in_ref.shape[1] // 2
    greet(rep_count, bit_count, replica, column)
    copies = {}

    def send(name, source, target, device):
        at = number[name]
        copies[name] = pltpu.make_async_remote_copy(
            src_ref=source, dst_ref=target, send_sem=send_sem.at[at], recv_sem=recv_sem.at[at],
            device_id=device, device_id_type=MESH,
        )
        copies[name].start()

    def bound_for(steps, col):
        return lax.rem(replica + steps, rep_count) * col_count + col

    def core_slot(steps, mask):
        return core_buf.at[steps * len(masks) + masks.index(mask)]

    def stage_slot(half, stage, steps, mask):
        left = submasks(orders[half][stage + 1 :])
        return stage_bufs[stage].at[(half * rep_count + steps) * len(left) + left.index(mask)]

    def held(half, stage, steps, mask):
        if stage == 0:
            return core_slot(steps, mask).at[pl.ds(half * half_rows, half_rows)]
        return stage_slot(half, stage - 1, steps, mask)

    for steps in shifts:
        for mask in masks:
            other = flipped(column, 0)
            send(("core", steps, mask), in_ref.at[bound_for(steps, masked(other, mask))], core_slot(steps, mask), (replica, other))

    def onward(half, stage, steps):
        if stage == stages:
            if steps:
                send(("rep", half, steps), held(half, stage, steps, 0), rep_buf.at[half * rep_count + steps], (lax.rem(replica + steps, rep_count), column))
            return
        bit = orders[half][stage]
        for mask in submasks(orders[half][stage + 1 :]):
            send((half, stage, steps, mask), held(half, stage, steps, mask | 1 << bit), stage_slot(half, stage, steps, mask), (replica, flipped(column, bit)))

    def take_core(steps):
        for mask in masks:
            copies[("core", steps, mask)].wait_recv()
            slot = core_slot(steps, mask)
            slot[...] = slot[...] + in_ref[bound_for(steps, masked(column, mask))]
        for half in range(2):
            onward(half, 0, steps)

    def take_stage(stage, steps):
        for half in range(2):
            for mask in submasks(orders[half][stage + 1 :]):
                copies[(half, stage, steps, mask)].wait_recv()
                slot = stage_slot(half, stage, steps, mask)
                slot[...] = slot[...] + held(half, stage, steps, mask)[...]
            onward(half, stage + 1, steps)

    for turn in range(rep_count + stages):
        if turn < rep_count:
            take_core(shifts[turn])
        for stage in range(stages):
            if 0 <= turn - stage - 1 < rep_count:
                take_stage(stage, shifts[turn - stage - 1])
    for half in range(2):
        total = held(half, stages, 0, 0)[...].astype(jnp.float32)
        for steps in range(1, rep_count):
            copies[("rep", half, steps)].wait_recv()
            total = total + rep_buf[half * rep_count + steps].astype(jnp.float32)
        out_ref[pl.ds(half * half_rows, half_rows)] = total.astype(out_ref.dtype)
    for copy in copies.values():
        copy.wait_send()


def scatter_sum(partial, rep_count, col_count, out_dtype, collective_id):
    bit_count = col_count.bit_length() - 1
    orders, shifts, masks, number = scatter_plan(rep_count, bit_count)
    blocks = rep_count * col_count
    rows, width = partial.shape[0] // blocks, partial.shape[1]
    half = rows // 2
    buffers = [pltpu.VMEM((rep_count * len(masks), rows, width), partial.dtype)]
    for stage in range(bit_count - 1):
        buffers.append(pltpu.VMEM((2 * rep_count * len(masks) >> stage + 1, half, width), partial.dtype))
    buffers.append(pltpu.VMEM((2 * rep_count, half, width), partial.dtype))
    size = rows * width * 2
    return pl.pallas_call(
        functools.partial(scatter_kernel, rep_count, col_count),
        out_shape=jax.ShapeDtypeStruct((rows, width), out_dtype),
        in_specs=[pl.BlockSpec(memory_space=pltpu.VMEM)],
        out_specs=pl.BlockSpec(memory_space=pltpu.VMEM),
        scratch_shapes=buffers
        + [pltpu.SemaphoreType.DMA((len(number),)), pltpu.SemaphoreType.DMA((len(number),))],
        compiler_params=pltpu.CompilerParams(
            collective_id=collective_id,
            has_side_effects=True,
            vmem_limit_bytes=size * (2 * blocks + rep_count + 4) + (2 << 20),
        ),
    )(partial.reshape(blocks, rows, width))


PAIR = 2 * KVW // 128
KEYW = -(-KVW // 128) * 128


def split_pairs(flat, row, stride_rows, count):
    tiles = [flat[pl.ds(stride_rows * j + row, count, stride=stride_rows * PAIR), :] for j in range(PAIR)]
    low = lax.broadcasted_iota(jnp.int32, (count, 128), 1) < 64
    half = PAIR // 2
    turned = [pltpu.roll(tile, 64, 1) for tile in tiles[half:]]
    even = tiles[:half] + [jnp.where(low, tiles[half], 0.0)]
    odd = [jnp.where(low, turned[c], turned[c + 1]) for c in range(half)] + [jnp.where(low, turned[half], 0.0)]
    return even, odd


def widen(source, rows, flat, pairs):
    def step(at, carry):
        base = pl.multiple_of(at * PAIR * 128, 128)
        block = source[rows, pl.ds(base, PAIR * 128)].astype(jnp.float32)
        for j in range(PAIR):
            flat[pl.ds(pl.multiple_of((at * PAIR + j) * 8, 8), 8), :] = block[:, j * 128 : (j + 1) * 128]
        return carry

    lax.fori_loop(0, pairs, step, 0, unroll=4)


def attend_kernel(
    col_count, count_ref, fill_ref, order_ref, pages_ref, query_ref, out_ref,
    page_flat, query_flat, paged, keys, raw, order_mat, held, send_sem, recv_sem, local_sem,
):
    request_count = REQ_DEV
    row_count = SPEC * HEADS
    replica, column = lax.axis_index("rep"), lax.axis_index("ep")
    block_rows = row_count // col_count
    heads_dev = block_rows // SPEC
    barrier = pltpu.get_barrier_semaphore()
    for steps in range(1, col_count):
        pl.semaphore_signal(barrier, inc=1, device_id=(replica, lax.rem(column + steps, col_count)), device_id_type=MESH)

    row = lax.broadcasted_iota(jnp.int32, (row_count, row_count), 0)
    place = lax.broadcasted_iota(jnp.int32, (row_count, row_count), 1)
    head = row // block_rows * heads_dev + row % heads_dev
    spot = row % block_rows // heads_dev
    wanted = head % 2 * (row_count // 2) + (spot * HEADS + head) // 2
    order_mat[...] = jnp.where(place == wanted, 1.0, 0.0).astype(jnp.bfloat16)

    def group_step(group, carry):
        widen(pages_ref, pl.ds(pl.multiple_of(group * 8, 8), 8), page_flat, PAGE // 2)

        def page_step(page, carry):
            even, odd = split_pairs(page_flat, page, 8, PAGE // 2)
            for c in range(KEYW // 128):
                lanes = pl.ds(c * 128, 128)
                paged[group * 8 + page, pl.ds(0, PAGE // 2), lanes] = even[c].astype(jnp.bfloat16)
                paged[group * 8 + page, pl.ds(PAGE // 2, PAGE // 2), lanes] = odd[c].astype(jnp.bfloat16)
            return carry

        lax.fori_loop(0, 8, page_step, 0)
        return carry

    lax.fori_loop(0, PAGES_DEV // 8, group_step, 0)
    widen(query_ref, slice(None), query_flat, row_count // 2)
    pl.semaphore_wait(barrier, col_count - 1)

    def copy_of(request, steps):
        there = lax.rem(column + steps, col_count)
        return pltpu.make_async_remote_copy(
            src_ref=held.at[request, there], dst_ref=out_ref.at[column, request],
            send_sem=send_sem.at[request, steps], recv_sem=recv_sem.at[request, steps],
            device_id=(replica, there), device_id_type=MESH,
        )

    def own_copy(request):
        return pltpu.make_async_copy(held.at[request, column], out_ref.at[column, request], local_sem.at[request])

    def step(request, offset):
        count = count_ref[replica, 0, request]
        length = (count - 1) * PAGE + fill_ref[replica, 0, request]
        for page in range(MAXP):
            at = order_ref[0, jnp.minimum(offset + page, PAGES_DEV - 1)]
            keys[pl.ds(page * PAGE, PAGE), :] = paged[at]
        even, odd = split_pairs(query_flat, request, 8, row_count // 2)
        for c in range(KEYW // 128):
            lanes = pl.ds(c * 128, 128)
            raw[pl.ds(0, row_count // 2), lanes] = even[c].astype(jnp.bfloat16)
            raw[pl.ds(row_count // 2, row_count // 2), lanes] = odd[c].astype(jnp.bfloat16)
        query = jnp.dot(order_mat[...], raw[...], preferred_element_type=jnp.float32).astype(jnp.bfloat16)
        scores = lax.dot_general(query, keys[...], (((1,), (1,)), ((), ())), preferred_element_type=jnp.float32)
        entry = lax.broadcasted_iota(jnp.int32, (1, MAXP * PAGE), 1)
        inside = entry % PAGE
        position = entry - inside + inside % (PAGE // 2) * 2 + inside // (PAGE // 2)
        spare = lax.broadcasted_iota(jnp.int32, (row_count, 1), 0) % block_rows // heads_dev
        scores = jnp.where(position < length - SPEC + 1 + spare, scores, -1e30)
        exponent = jnp.exp((scores - jnp.max(scores, axis=1, keepdims=True)) * SCORE_SCALE)
        probability = (exponent * (1.0 / jnp.sum(exponent, axis=1, keepdims=True))).astype(jnp.bfloat16)
        latent = jnp.dot(probability, keys[:, :LAT], preferred_element_type=jnp.float32)
        held[request] = latent.astype(jnp.bfloat16).reshape(col_count, block_rows, LAT)
        for steps in range(1, col_count):
            copy_of(request, steps).start()
        own_copy(request).start()
        return offset + count

    lax.fori_loop(0, request_count, step, 0)

    def finish(request, carry):
        for steps in range(1, col_count):
            copy_of(request, steps).wait()
        own_copy(request).wait()
        return carry

    lax.fori_loop(0, request_count, finish, 0)


def attend(pages, queries, counts, fills, order, col_count, collective_id):
    request_count = queries.shape[0]
    row_count = SPEC * HEADS
    block_rows = row_count // col_count
    return pl.pallas_call(
        functools.partial(attend_kernel, col_count),
        out_shape=jax.ShapeDtypeStruct((col_count, request_count, block_rows, LAT), jnp.bfloat16),
        in_specs=[pl.BlockSpec(memory_space=pltpu.SMEM)] * 3 + [pl.BlockSpec(memory_space=pltpu.VMEM)] * 2,
        out_specs=pl.BlockSpec(memory_space=pltpu.VMEM),
        scratch_shapes=[
            pltpu.VMEM((8 * PAGE * KVW // 128, 128), jnp.float32),
            pltpu.VMEM((8 * row_count * KVW // 128, 128), jnp.float32),
            pltpu.VMEM((PAGES_DEV, PAGE, KEYW), jnp.bfloat16),
            pltpu.VMEM((MAXP * PAGE, KEYW), jnp.bfloat16),
            pltpu.VMEM((row_count, KEYW), jnp.bfloat16),
            pltpu.VMEM((row_count, row_count), jnp.bfloat16),
            pltpu.VMEM((request_count, col_count, block_rows, LAT), jnp.bfloat16),
            pltpu.SemaphoreType.DMA((request_count, col_count)),
            pltpu.SemaphoreType.DMA((request_count, col_count)),
            pltpu.SemaphoreType.DMA((request_count,)),
        ],
        compiler_params=pltpu.CompilerParams(
            collective_id=collective_id, has_side_effects=True, vmem_limit_bytes=36 << 20
        ),
    )(counts, fills, order, pages, queries)


def swap_kernel(rep_count, in_ref, out_ref, send_sem, recv_sem):
    replica, column = lax.axis_index("rep"), lax.axis_index("ep")
    greet(rep_count, 0, replica, column)
    copies = []
    for steps in range(1, rep_count):
        copies.append(
            pltpu.make_async_remote_copy(
                src_ref=in_ref, dst_ref=out_ref.at[steps - 1],
                send_sem=send_sem.at[steps], recv_sem=recv_sem.at[steps],
                device_id=(lax.rem(replica + steps, rep_count), column), device_id_type=MESH,
            )
        )
        copies[-1].start()
    for copy in copies:
        copy.wait()


def swap(rows, rep_count, collective_id):
    return pl.pallas_call(
        functools.partial(swap_kernel, rep_count),
        out_shape=jax.ShapeDtypeStruct((rep_count - 1,) + rows.shape, rows.dtype),
        in_specs=[pl.BlockSpec(memory_space=pltpu.VMEM)],
        out_specs=pl.BlockSpec(memory_space=pltpu.VMEM),
        scratch_shapes=[pltpu.SemaphoreType.DMA((rep_count,)), pltpu.SemaphoreType.DMA((rep_count,))],
        compiler_params=pltpu.CompilerParams(
            collective_id=collective_id, has_side_effects=True, vmem_limit_bytes=8 << 20
        ),
    )(rows)


def served_rows(own_rows, own_sheds, shifts):
    rep_count = lax.axis_size("rep")
    hits = own_sheds[:, None] == jnp.arange(REQ_DEV, dtype=jnp.int32)[None, :]
    leaving = [jnp.sum(jnp.where(hits[k][:, None], own_rows, 0), axis=0, keepdims=True) for k in range(own_sheds.shape[0])]
    leaving = jnp.concatenate(leaving, axis=0)
    arrived = leaving
    for steps in range(1, rep_count):
        moved = shifted(leaving, "rep", steps)
        arrived = jnp.where((shifts == steps)[:, None], moved, arrived)
    served = own_rows
    for k in range(own_sheds.shape[0]):
        served = jnp.where(hits[k][:, None], arrived[k][None, :], served)
    return served


def served_tokens(own_tokens, own_sheds, shifts, collective_id):
    rep_count = lax.axis_size("rep")
    owner = jnp.arange(own_tokens.shape[0], dtype=jnp.int32) // SPEC
    hits = own_sheds[:, None] == owner[None, :]
    width = own_tokens.shape[1]
    blocks = own_tokens.reshape(REQ_DEV, SPEC, width)
    shed = own_sheds.shape[0]
    block_hits = own_sheds[:, None] == jnp.arange(REQ_DEV, dtype=jnp.int32)[None, :]
    leaving = jnp.sum(jnp.where(block_hits[:, :, None, None], blocks[None], 0), axis=1)
    moved = swap(leaving.reshape(shed * SPEC, width), rep_count, collective_id)
    moved = moved.reshape(rep_count - 1, shed, SPEC, width)
    arrived = moved[0]
    for steps in range(2, rep_count):
        arrived = jnp.where((shifts == steps)[:, None, None], moved[steps - 1], arrived)
    served = own_tokens
    for k in range(shed):
        repeated = jnp.tile(arrived[k], (REQ_DEV, 1))
        served = jnp.where(hits[k][:, None], repeated, served)
    return served


def gate_columns(expert_ids, gate_weight, expert_home, device_count):
    target = jnp.sum(
        jnp.where(
            expert_ids[:, :, None] == jnp.arange(device_count, dtype=jnp.int32)[None, None, :],
            expert_home[None, None, :],
            0,
        ),
        axis=2,
    )
    return jnp.sum(
        jnp.where(
            target[:, :, None] == jnp.arange(device_count, dtype=jnp.int32)[None, None, :],
            gate_weight[:, :, None],
            0.0,
        ),
        axis=1,
    )


def per_device(
    latent_pages,
    queries,
    residual,
    page_count,
    last_fill,
    page_order,
    shed_slots,
    shed_shift,
    expert_ids,
    gate_weight,
    expert_home,
    norm_gain,
    value_up,
    out_weight,
    expert_in,
    expert_out,
):
    rep_count = lax.axis_size("rep")
    col_count = lax.axis_size("ep")
    device_count = rep_count * col_count
    replica = lax.axis_index("rep")
    me = replica * col_count + lax.axis_index("ep")
    own_sheds = shed_slots[replica, 0, :]
    shifts = shed_shift[0]
    served_residual = served_rows(residual, own_sheds, shifts)
    gates = gate_columns(expert_ids, gate_weight, expert_home, device_count)
    gates_high = gates.astype(jnp.bfloat16)
    gates_low = (gates - gates_high.astype(jnp.float32)).astype(jnp.bfloat16)

    tokens_dev = REQ_DEV * SPEC
    heads_dev = value_up.shape[0]
    regrouped = attend(latent_pages, queries, page_count, last_fill, page_order, col_count, 3)
    row_block = regrouped.reshape(tokens_dev * col_count, heads_dev, LAT)
    lifted = jnp.einsum(
        "thl,hlv->thv", row_block, value_up, preferred_element_type=jnp.float32
    ).astype(jnp.bfloat16)
    own_branch = scatter_sum(
        jnp.dot(
            lifted.reshape(tokens_dev * col_count, heads_dev * VHEAD),
            out_weight,
            preferred_element_type=jnp.float32,
        ).astype(jnp.bfloat16),
        1,
        col_count,
        jnp.bfloat16,
        0,
    )
    served_branch = served_tokens(own_branch, own_sheds, shifts, 4)
    attn_proj = served_branch.reshape(REQ_DEV, SPEC * D)
    branch = served_branch.astype(jnp.float32)
    mixed = served_residual.reshape(tokens_dev, D).astype(jnp.float32) + branch
    square = jnp.mean(mixed * mixed, axis=1, keepdims=True)
    normed = (mixed * lax.rsqrt(square + NORM_EPS) * norm_gain).astype(jnp.bfloat16)
    spare = -2 * device_count % 128
    packed = jnp.concatenate(
        (normed, gates_high, gates_low, jnp.zeros((tokens_dev, spare), jnp.bfloat16)), axis=1
    )
    everyone = gather_all(packed, rep_count, col_count, 1)
    all_gates = everyone[:, D : D + 2 * device_count].astype(jnp.float32)
    picks = jnp.arange(2 * device_count, dtype=jnp.int32) % device_count == me
    gate = jnp.sum(jnp.where(picks[None, :], all_gates, 0.0), axis=1, keepdims=True)
    inner_act = jax.nn.silu(
        jnp.dot(everyone[:, :D], expert_in[0], preferred_element_type=jnp.float32)
    ).astype(jnp.bfloat16)
    outer_out = jnp.dot(inner_act, expert_out[0], preferred_element_type=jnp.float32)
    moe_sum = scatter_sum(
        (gate * outer_out).astype(jnp.bfloat16), rep_count, col_count, jnp.float32, 2
    )
    layer_out = (mixed + moe_sum).astype(jnp.bfloat16).reshape(REQ_DEV, SPEC * D)
    return (attn_proj, layer_out)


def solution(mesh):
    placed = (
        P(("rep", "ep"), None),
        P(("rep", "ep"), None),
        P(("rep", "ep"), None),
        P(None, "ep", None),
        P(None, "ep", None),
        P(("rep", "ep"), None),
        P(None, "ep", None),
        P("ep", None),
        P(("rep", "ep"), None),
        P(("rep", "ep"), None),
        P(),
        P(),
        P("ep", None, None),
        P("ep", None),
        P(("rep", "ep"), None, None),
        P(("rep", "ep"), None, None),
    )
    return jax.shard_map(
        per_device,
        mesh=mesh,
        in_specs=placed,
        out_specs=(P(("rep", "ep"), None), P(("rep", "ep"), None)),
        check_vma=False,
    )
```

```python
import functools

import jax
import jax.numpy as jnp
from jax import lax
from jax.experimental import pallas as pl
from jax.experimental.pallas import tpu as pltpu
from jax.sharding import PartitionSpec as P

D = 3584
HEADS = 64
LAT = 512
KVW = 576
VHEAD = 128
TOP = 8
PAGE = 64
SPEC = 4
MAXP = 12
REQ_DEV = 8
PAGES_DEV = 48


SCORE_SCALE = 192.0 ** (-0.5)
NORM_EPS = 0.25
MESH = pl.DeviceIdType.MESH


def shifted(value, axis, steps):
    count = lax.axis_size(axis)
    pairs = [(source, (source + steps) % count) for source in range(count)]
    return lax.ppermute(value, axis, pairs)


def flipped(index, bit):
    width = 1 << bit
    return index + width * (1 - 2 * ((index // width) % 2))


def masked(index, mask):
    for bit in range(mask.bit_length()):
        if mask >> bit & 1:
            index = flipped(index, bit)
    return index


def submasks(bits):
    masks = [0]
    for bit in bits:
        masks = masks + [mask | 1 << bit for mask in masks]
    return masks


def greet(rep_count, bit_count, replica, column):
    barrier = pltpu.get_barrier_semaphore()
    for steps in range(1, rep_count):
        pl.semaphore_signal(barrier, inc=1, device_id=(lax.rem(replica + steps, rep_count), column), device_id_type=MESH)
    for bit in range(bit_count):
        pl.semaphore_signal(barrier, inc=1, device_id=(replica, flipped(column, bit)), device_id_type=MESH)
    pl.semaphore_wait(barrier, rep_count - 1 + bit_count)


def gather_plan(rep_count, bit_count):
    outer = list(range(1, bit_count))
    orders = (outer, outer[::-1])
    names = [("rep", steps) for steps in range(1, rep_count)]
    for half in range(2):
        for stage in range(len(outer)):
            for steps in range(rep_count):
                names += [(half, stage, steps, mask) for mask in submasks(orders[half][:stage])]
        for steps in range(rep_count):
            names += [("core", half, steps, mask) for mask in submasks(outer)]
    return orders, {name: at for at, name in enumerate(names)}


def gather_kernel(rep_count, col_count, in_ref, out_ref, send_sem, recv_sem, local_sem):
    bit_count = col_count.bit_length() - 1
    replica, column = lax.axis_index("rep"), lax.axis_index("ep")
    orders, number = gather_plan(rep_count, bit_count)
    half_rows = in_ref.shape[0] // 2
    greet(rep_count, bit_count, replica, column)

    def block(steps, mask, half):
        rows = slice(None) if half is None else pl.ds(half * half_rows, half_rows)
        origin = lax.rem(replica + rep_count - steps, rep_count)
        return out_ref.at[origin * col_count + masked(column, mask), rows]

    own = replica * col_count + column
    copies = {}

    def send(name, source, target, device):
        at = number[name]
        copies[name] = pltpu.make_async_remote_copy(
            src_ref=source, dst_ref=target, send_sem=send_sem.at[at], recv_sem=recv_sem.at[at],
            device_id=device, device_id_type=MESH,
        )
        copies[name].start()

    def spread(steps, half, mask, done):
        rows = pl.ds(half * half_rows, half_rows)
        source = in_ref.at[rows] if steps == 0 and mask == 0 else block(steps, mask, half)
        for stage in range(done, len(orders[half])):
            send((half, stage, steps, mask), source, block(steps, mask, half), (replica, flipped(column, orders[half][stage])))
        send(("core", half, steps, mask), source, block(steps, mask, half), (replica, flipped(column, 0)))

    for steps in range(1, rep_count):
        send(("rep", steps), in_ref, out_ref.at[own], (lax.rem(replica + steps, rep_count), column))
    for half in range(2):
        spread(0, half, 0, 0)
    mine = pltpu.make_async_copy(in_ref, out_ref.at[own], local_sem)
    mine.start()

    def arrivals(stage, steps):
        for half in range(2):
            bit = orders[half][stage]
            for mask in submasks(orders[half][:stage]):
                copies[(half, stage, steps, mask)].wait_recv()
                spread(steps, half, mask | 1 << bit, stage + 1)

    stages = len(orders[0])
    for turn in range(rep_count + stages):
        if 0 < turn < rep_count:
            copies[("rep", turn)].wait_recv()
            for half in range(2):
                spread(turn, half, 0, 0)
        for stage in range(stages):
            if 0 <= turn - stage < rep_count:
                arrivals(stage, turn - stage)
    mine.wait()
    for name, copy in copies.items():
        if name[0] == "core":
            copy.wait_recv()
        copy.wait_send()


def gather_all(rows, rep_count, col_count, collective_id):
    _, number = gather_plan(rep_count, col_count.bit_length() - 1)
    blocks = rep_count * col_count
    size = rows.size * 2
    out = pl.pallas_call(
        functools.partial(gather_kernel, rep_count, col_count),
        out_shape=jax.ShapeDtypeStruct((blocks,) + rows.shape, rows.dtype),
        in_specs=[pl.BlockSpec(memory_space=pltpu.VMEM)],
        out_specs=pl.BlockSpec(memory_space=pltpu.VMEM),
        scratch_shapes=[
            pltpu.SemaphoreType.DMA((len(number),)),
            pltpu.SemaphoreType.DMA((len(number),)),
            pltpu.SemaphoreType.DMA,
        ],
        compiler_params=pltpu.CompilerParams(
            collective_id=collective_id, has_side_effects=True, vmem_limit_bytes=size * (blocks + 2) + (2 << 20)
        ),
    )(rows)
    return out.reshape(blocks * rows.shape[0], rows.shape[1])


def scatter_plan(rep_count, bit_count):
    outer = list(range(1, bit_count))
    orders = (outer[::-1], outer)
    shifts = list(range(1, rep_count)) + [0]
    masks = sorted(submasks(outer), key=lambda mask: -bin(mask).count("1"))
    names = [("core", steps, mask) for steps in shifts for mask in masks]
    for half in range(2):
        for stage in range(len(outer)):
            for steps in shifts:
                names += [(half, stage, steps, mask) for mask in submasks(orders[half][stage + 1 :])]
        names += [("rep", half, steps) for steps in range(1, rep_count)]
    return orders, shifts, masks, {name: at for at, name in enumerate(names)}


def scatter_kernel(rep_count, col_count, in_ref, out_ref, core_buf, *rest):
    bit_count = col_count.bit_length() - 1
    stages = bit_count - 1
    stage_bufs, (rep_buf, send_sem, recv_sem) = rest[:stages], rest[stages:]
    replica, column = lax.axis_index("rep"), lax.axis_index("ep")
    orders, shifts, masks, number = scatter_plan(rep_count, bit_count)
    half_rows = in_ref.shape[1] // 2
    greet(rep_count, bit_count, replica, column)
    copies = {}

    def send(name, source, target, device):
        at = number[name]
        copies[name] = pltpu.make_async_remote_copy(
            src_ref=source, dst_ref=target, send_sem=send_sem.at[at], recv_sem=recv_sem.at[at],
            device_id=device, device_id_type=MESH,
        )
        copies[name].start()

    def bound_for(steps, col):
        return lax.rem(replica + steps, rep_count) * col_count + col

    def core_slot(steps, mask):
        return core_buf.at[steps * len(masks) + masks.index(mask)]

    def stage_slot(half, stage, steps, mask):
        left = submasks(orders[half][stage + 1 :])
        return stage_bufs[stage].at[(half * rep_count + steps) * len(left) + left.index(mask)]

    def held(half, stage, steps, mask):
        if stage == 0:
            return core_slot(steps, mask).at[pl.ds(half * half_rows, half_rows)]
        return stage_slot(half, stage - 1, steps, mask)

    for steps in shifts:
        for mask in masks:
            other = flipped(column, 0)
            send(("core", steps, mask), in_ref.at[bound_for(steps, masked(other, mask))], core_slot(steps, mask), (replica, other))

    def onward(half, stage, steps):
        if stage == stages:
            if steps:
                send(("rep", half, steps), held(half, stage, steps, 0), rep_buf.at[half * rep_count + steps], (lax.rem(replica + steps, rep_count), column))
            return
        bit = orders[half][stage]
        for mask in submasks(orders[half][stage + 1 :]):
            send((half, stage, steps, mask), held(half, stage, steps, mask | 1 << bit), stage_slot(half, stage, steps, mask), (replica, flipped(column, bit)))

    def take_core(steps):
        for mask in masks:
            copies[("core", steps, mask)].wait_recv()
            slot = core_slot(steps, mask)
            slot[...] = slot[...] + in_ref[bound_for(steps, masked(column, mask))]
        for half in range(2):
            onward(half, 0, steps)

    def take_stage(stage, steps):
        for half in range(2):
            for mask in submasks(orders[half][stage + 1 :]):
                copies[(half, stage, steps, mask)].wait_recv()
                slot = stage_slot(half, stage, steps, mask)
                slot[...] = slot[...] + held(half, stage, steps, mask)[...]
            onward(half, stage + 1, steps)

    for turn in range(rep_count + stages):
        if turn < rep_count:
            take_core(shifts[turn])
        for stage in range(stages):
            if 0 <= turn - stage - 1 < rep_count:
                take_stage(stage, shifts[turn - stage - 1])
    for half in range(2):
        total = held(half, stages, 0, 0)[...].astype(jnp.float32)
        for steps in range(1, rep_count):
            copies[("rep", half, steps)].wait_recv()
            total = total + rep_buf[half * rep_count + steps].astype(jnp.float32)
        out_ref[pl.ds(half * half_rows, half_rows)] = total.astype(out_ref.dtype)
    for copy in copies.values():
        copy.wait_send()


def scatter_sum(partial, rep_count, col_count, out_dtype, collective_id):
    bit_count = col_count.bit_length() - 1
    orders, shifts, masks, number = scatter_plan(rep_count, bit_count)
    blocks = rep_count * col_count
    rows, width = partial.shape[0] // blocks, partial.shape[1]
    half = rows // 2
    buffers = [pltpu.VMEM((rep_count * len(masks), rows, width), partial.dtype)]
    for stage in range(bit_count - 1):
        buffers.append(pltpu.VMEM((2 * rep_count * len(masks) >> stage + 1, half, width), partial.dtype))
    buffers.append(pltpu.VMEM((2 * rep_count, half, width), partial.dtype))
    size = rows * width * 2
    return pl.pallas_call(
        functools.partial(scatter_kernel, rep_count, col_count),
        out_shape=jax.ShapeDtypeStruct((rows, width), out_dtype),
        in_specs=[pl.BlockSpec(memory_space=pltpu.VMEM)],
        out_specs=pl.BlockSpec(memory_space=pltpu.VMEM),
        scratch_shapes=buffers
        + [pltpu.SemaphoreType.DMA((len(number),)), pltpu.SemaphoreType.DMA((len(number),))],
        compiler_params=pltpu.CompilerParams(
            collective_id=collective_id,
            has_side_effects=True,
            vmem_limit_bytes=size * (2 * blocks + rep_count + 4) + (2 << 20),
        ),
    )(partial.reshape(blocks, rows, width))


PAIR = 2 * KVW // 128
KEYW = -(-KVW // 128) * 128


def split_pairs(flat, row, stride_rows, count):
    tiles = [flat[pl.ds(stride_rows * j + row, count, stride=stride_rows * PAIR), :] for j in range(PAIR)]
    low = lax.broadcasted_iota(jnp.int32, (count, 128), 1) < 64
    half = PAIR // 2
    turned = [pltpu.roll(tile, 64, 1) for tile in tiles[half:]]
    even = tiles[:half] + [jnp.where(low, tiles[half], 0.0)]
    odd = [jnp.where(low, turned[c], turned[c + 1]) for c in range(half)] + [jnp.where(low, turned[half], 0.0)]
    return even, odd


def widen(source, rows, flat, pairs):
    def step(at, carry):
        base = pl.multiple_of(at * PAIR * 128, 128)
        block = source[rows, pl.ds(base, PAIR * 128)].astype(jnp.float32)
        for j in range(PAIR):
            flat[pl.ds(pl.multiple_of((at * PAIR + j) * 8, 8), 8), :] = block[:, j * 128 : (j + 1) * 128]
        return carry

    lax.fori_loop(0, pairs, step, 0, unroll=4)


def attend_kernel(
    col_count, count_ref, fill_ref, order_ref, pages_ref, query_ref, out_ref,
    page_flat, query_flat, paged, keys, raw, order_mat, held, send_sem, recv_sem, local_sem,
):
    request_count = REQ_DEV
    row_count = SPEC * HEADS
    replica, column = lax.axis_index("rep"), lax.axis_index("ep")
    block_rows = row_count // col_count
    heads_dev = block_rows // SPEC
    barrier = pltpu.get_barrier_semaphore()
    for steps in range(1, col_count):
        pl.semaphore_signal(barrier, inc=1, device_id=(replica, lax.rem(column + steps, col_count)), device_id_type=MESH)

    row = lax.broadcasted_iota(jnp.int32, (row_count, row_count), 0)
    place = lax.broadcasted_iota(jnp.int32, (row_count, row_count), 1)
    head = row // block_rows * heads_dev + row % heads_dev
    spot = row % block_rows // heads_dev
    wanted = head % 2 * (row_count // 2) + (spot * HEADS + head) // 2
    order_mat[...] = jnp.where(place == wanted, 1.0, 0.0).astype(jnp.bfloat16)

    def group_step(group, carry):
        widen(pages_ref, pl.ds(pl.multiple_of(group * 8, 8), 8), page_flat, PAGE // 2)

        def page_step(page, carry):
            even, odd = split_pairs(page_flat, page, 8, PAGE // 2)
            for c in range(KEYW // 128):
                lanes = pl.ds(c * 128, 128)
                paged[group * 8 + page, pl.ds(0, PAGE // 2), lanes] = even[c].astype(jnp.bfloat16)
                paged[group * 8 + page, pl.ds(PAGE // 2, PAGE // 2), lanes] = odd[c].astype(jnp.bfloat16)
            return carry

        lax.fori_loop(0, 8, page_step, 0)
        return carry

    lax.fori_loop(0, PAGES_DEV // 8, group_step, 0)
    widen(query_ref, slice(None), query_flat, row_count // 2)
    pl.semaphore_wait(barrier, col_count - 1)

    def copy_of(request, steps):
        there = lax.rem(column + steps, col_count)
        return pltpu.make_async_remote_copy(
            src_ref=held.at[request, there], dst_ref=out_ref.at[column, request],
            send_sem=send_sem.at[request, steps], recv_sem=recv_sem.at[request, steps],
            device_id=(replica, there), device_id_type=MESH,
        )

    def own_copy(request):
        return pltpu.make_async_copy(held.at[request, column], out_ref.at[column, request], local_sem.at[request])

    def step(request, offset):
        count = count_ref[replica, 0, request]
        length = (count - 1) * PAGE + fill_ref[replica, 0, request]
        for page in range(MAXP):
            at = order_ref[0, jnp.minimum(offset + page, PAGES_DEV - 1)]
            keys[pl.ds(page * PAGE, PAGE), :] = paged[at]
        even, odd = split_pairs(query_flat, request, 8, row_count // 2)
        for c in range(KEYW // 128):
            lanes = pl.ds(c * 128, 128)
            raw[pl.ds(0, row_count // 2), lanes] = even[c].astype(jnp.bfloat16)
            raw[pl.ds(row_count // 2, row_count // 2), lanes] = odd[c].astype(jnp.bfloat16)
        query = jnp.dot(order_mat[...], raw[...], preferred_element_type=jnp.float32).astype(jnp.bfloat16)
        scores = lax.dot_general(query, keys[...], (((1,), (1,)), ((), ())), preferred_element_type=jnp.float32)
        entry = lax.broadcasted_iota(jnp.int32, (1, MAXP * PAGE), 1)
        inside = entry % PAGE
        position = entry - inside + inside % (PAGE // 2) * 2 + inside // (PAGE // 2)
        spare = lax.broadcasted_iota(jnp.int32, (row_count, 1), 0) % block_rows // heads_dev
        scores = jnp.where(position < length - SPEC + 1 + spare, scores, -1e30)
        exponent = jnp.exp((scores - jnp.max(scores, axis=1, keepdims=True)) * SCORE_SCALE)
        probability = (exponent * (1.0 / jnp.sum(exponent, axis=1, keepdims=True))).astype(jnp.bfloat16)
        latent = jnp.dot(probability, keys[:, :LAT], preferred_element_type=jnp.float32)
        held[request] = latent.astype(jnp.bfloat16).reshape(col_count, block_rows, LAT)
        for steps in range(1, col_count):
            copy_of(request, steps).start()
        own_copy(request).start()
        return offset + count

    lax.fori_loop(0, request_count, step, 0)

    def finish(request, carry):
        for steps in range(1, col_count):
            copy_of(request, steps).wait()
        own_copy(request).wait()
        return carry

    lax.fori_loop(0, request_count, finish, 0)


def attend(pages, queries, counts, fills, order, col_count, collective_id):
    request_count = queries.shape[0]
    row_count = SPEC * HEADS
    block_rows = row_count // col_count
    return pl.pallas_call(
        functools.partial(attend_kernel, col_count),
        out_shape=jax.ShapeDtypeStruct((col_count, request_count, block_rows, LAT), jnp.bfloat16),
        in_specs=[pl.BlockSpec(memory_space=pltpu.SMEM)] * 3 + [pl.BlockSpec(memory_space=pltpu.VMEM)] * 2,
        out_specs=pl.BlockSpec(memory_space=pltpu.VMEM),
        scratch_shapes=[
            pltpu.VMEM((8 * PAGE * KVW // 128, 128), jnp.float32),
            pltpu.VMEM((8 * row_count * KVW // 128, 128), jnp.float32),
            pltpu.VMEM((PAGES_DEV, PAGE, KEYW), jnp.bfloat16),
            pltpu.VMEM((MAXP * PAGE, KEYW), jnp.bfloat16),
            pltpu.VMEM((row_count, KEYW), jnp.bfloat16),
            pltpu.VMEM((row_count, row_count), jnp.bfloat16),
            pltpu.VMEM((request_count, col_count, block_rows, LAT), jnp.bfloat16),
            pltpu.SemaphoreType.DMA((request_count, col_count)),
            pltpu.SemaphoreType.DMA((request_count, col_count)),
            pltpu.SemaphoreType.DMA((request_count,)),
        ],
        compiler_params=pltpu.CompilerParams(
            collective_id=collective_id, has_side_effects=True, vmem_limit_bytes=36 << 20
        ),
    )(counts, fills, order, pages, queries)


def swap_kernel(rep_count, in_ref, out_ref, send_sem, recv_sem):
    replica, column = lax.axis_index("rep"), lax.axis_index("ep")
    greet(rep_count, 0, replica, column)
    copies = []
    for steps in range(1, rep_count):
        copies.append(
            pltpu.make_async_remote_copy(
                src_ref=in_ref, dst_ref=out_ref.at[steps - 1],
                send_sem=send_sem.at[steps], recv_sem=recv_sem.at[steps],
                device_id=(lax.rem(replica + steps, rep_count), column), device_id_type=MESH,
            )
        )
        copies[-1].start()
    for copy in copies:
        copy.wait()


def swap(rows, rep_count, collective_id):
    return pl.pallas_call(
        functools.partial(swap_kernel, rep_count),
        out_shape=jax.ShapeDtypeStruct((rep_count - 1,) + rows.shape, rows.dtype),
        in_specs=[pl.BlockSpec(memory_space=pltpu.VMEM)],
        out_specs=pl.BlockSpec(memory_space=pltpu.VMEM),
        scratch_shapes=[pltpu.SemaphoreType.DMA((rep_count,)), pltpu.SemaphoreType.DMA((rep_count,))],
        compiler_params=pltpu.CompilerParams(
            collective_id=collective_id, has_side_effects=True, vmem_limit_bytes=8 << 20
        ),
    )(rows)


LEAD = 1
FIRST = 512
SECOND = 512


def moe_keys(bit_count):
    outer = list(range(1, bit_count))
    spread_orders = (outer, outer[::-1])
    reduce_orders = (outer[::-1], outer)
    masks = sorted(submasks(outer), key=lambda mask: -bin(mask).count("1"))
    keys = [("spread", "rep", 0, 0)]
    for half in range(2):
        for stage in range(len(outer)):
            keys += [("spread", half, stage, mask) for mask in submasks(spread_orders[half][:stage])]
        keys += [("spread", "core", half, mask) for mask in masks]
    keys += [("reduce", "core", 0, mask) for mask in masks]
    for half in range(2):
        for stage in range(len(outer)):
            keys += [("reduce", half, stage, mask) for mask in submasks(reduce_orders[half][stage + 1 :])]
        keys.append(("reduce", "rep", half, 0))
    return spread_orders, reduce_orders, masks, {key: at for at, key in enumerate(keys)}


def moe_kernel(
    rep_count, col_count, in_ref, in_weight, out_weight, out_ref,
    got, held_in, held_out, inner, gate, partial, core_buf, *rest,
):
    bit_count = col_count.bit_length() - 1
    stages = bit_count - 1
    stage_bufs, (rep_buf, send_sem, recv_sem, local_sem) = rest[:stages], rest[stages:]
    replica, column = lax.axis_index("rep"), lax.axis_index("ep")
    me = replica * col_count + column
    device_count = rep_count * col_count
    spread_orders, reduce_orders, masks, number = moe_keys(bit_count)
    rows = in_ref.shape[0]
    width = out_ref.shape[1]
    half_rows = rows // 2
    other = flipped(column, 0)
    loads = [
        pltpu.make_async_copy(in_weight.at[0], held_in, local_sem.at[1]),
        pltpu.make_async_copy(out_weight.at[0], held_out, local_sem.at[2]),
    ]
    for load in loads:
        load.start()
    greet(rep_count, bit_count, replica, column)

    def origin(steps):
        return lax.rem(replica + rep_count - steps, rep_count)

    def block(steps, mask, half):
        return got.at[origin(steps) * col_count + masked(column, mask), pl.ds(half * half_rows, half_rows)]

    def core_slot(steps, mask):
        return core_buf.at[steps * len(masks) + masks.index(mask)]

    def stage_slot(half, stage, steps, mask):
        left = submasks(reduce_orders[half][stage + 1 :])
        return stage_bufs[stage].at[(half * rep_count + steps) * len(left) + left.index(mask)]

    def partly(half, stage, steps, mask):
        if stage == 0:
            return core_slot(steps, mask).at[pl.ds(half * half_rows, half_rows)]
        return stage_slot(half, stage - 1, steps, mask)

    def copy_of(key, steps, source=None):
        way, kind, at, mask = key
        if way == "spread":
            if kind == "rep":
                ends = in_ref, got.at[me], (lax.rem(replica + steps, rep_count), column)
            elif kind == "core":
                ends = block(steps, mask, at), block(steps, mask, at), (replica, other)
            else:
                there = (replica, flipped(column, spread_orders[kind][at]))
                ends = block(steps, mask, kind), block(steps, mask, kind), there
        elif kind == "core":
            ends = partial.at[steps, masked(other, mask)], core_slot(steps, mask), (replica, other)
        elif kind == "rep":
            ends = partly(at, stages, steps, 0), rep_buf.at[at * rep_count + steps], (origin(steps), column)
        else:
            bit = reduce_orders[kind][at]
            there = (replica, flipped(column, bit))
            ends = partly(kind, at, steps, mask | 1 << bit), stage_slot(kind, at, steps, mask), there
        slot = number[key] * rep_count + steps
        return pltpu.make_async_remote_copy(
            src_ref=ends[0] if source is None else source, dst_ref=ends[1],
            send_sem=send_sem.at[slot], recv_sem=recv_sem.at[slot], device_id=ends[2], device_id_type=MESH,
        )

    def spread(steps, half, mask, done, source=None):
        for stage in range(done, stages):
            copy_of(("spread", half, stage, mask), steps, source).start()
        copy_of(("spread", "core", half, mask), steps, source).start()

    def take_rep(steps):
        copy_of(("spread", "rep", 0, 0), steps).wait_recv()
        for half in range(2):
            spread(steps, half, 0, 0)

    def take_spread(stage, steps):
        for half in range(2):
            bit = spread_orders[half][stage]
            for mask in submasks(spread_orders[half][:stage]):
                copy_of(("spread", half, stage, mask), steps).wait_recv()
                spread(steps, half, mask | 1 << bit, stage + 1)

    def take_all(steps):
        for half in range(2):
            for mask in masks:
                copy_of(("spread", "core", half, mask), steps).wait_recv()

    def onward(half, stage, steps):
        if stage == stages:
            @pl.when(steps != 0)
            def _():
                copy_of(("reduce", "rep", half, 0), steps).start()
            return
        for mask in submasks(reduce_orders[half][stage + 1 :]):
            copy_of(("reduce", half, stage, mask), steps).start()

    def take_core(steps):
        for mask in masks:
            copy_of(("reduce", "core", 0, mask), steps).wait_recv()
            slot = core_slot(steps, mask)
            slot[...] = slot[...] + partial[steps, masked(column, mask)]
        for half in range(2):
            onward(half, 0, steps)

    def take_reduce(stage, steps):
        for half in range(2):
            for mask in submasks(reduce_orders[half][stage + 1 :]):
                copy_of(("reduce", half, stage, mask), steps).wait_recv()
                slot = stage_slot(half, stage, steps, mask)
                slot[...] = slot[...] + partly(half, stage, steps, mask)[...]
            onward(half, stage + 1, steps)

    for steps in range(1, rep_count):
        copy_of(("spread", "rep", 0, 0), steps).start()
    for half in range(2):
        spread(0, half, 0, 0, in_ref.at[pl.ds(half * half_rows, half_rows)])
    mine = pltpu.make_async_copy(in_ref, got.at[me], local_sem.at[0])
    mine.start()
    for steps in range(LEAD + 1):
        for stage in range(stages):
            take_spread(stage, steps)
            if stage == 0 and steps + 1 < rep_count:
                take_rep(steps + 1)
        if steps == 0:
            mine.wait()
            for load in loads:
                load.wait()
        take_all(steps)

    tall = col_count * rows

    def first(steps, chunk):
        tokens = got[pl.ds(origin(steps) * col_count, col_count), :, pl.ds(0, width)].reshape(tall, width)
        lanes = pl.ds(chunk * FIRST, FIRST)
        hidden = jnp.dot(tokens, held_in[:, lanes], preferred_element_type=jnp.float32)
        inner[:, lanes] = (hidden / (1.0 + jnp.exp(-hidden))).astype(jnp.bfloat16)

    def weigh(steps):
        spare = in_ref.shape[1] - width
        listed = got[pl.ds(origin(steps) * col_count, col_count), :, pl.ds(width, spare)].reshape(tall, spare)
        lane = lax.broadcasted_iota(jnp.int32, (tall, spare), 1)
        mine = (lane % device_count == me) & (lane < 2 * device_count)
        gate[...] = jnp.sum(jnp.where(mine, listed.astype(jnp.float32), 0.0), axis=1, keepdims=True)

    def second(steps, chunk):
        lanes = pl.ds(chunk * SECOND, SECOND)
        outer = jnp.dot(inner[...], held_out[:, lanes], preferred_element_type=jnp.float32)
        partial[steps, :, :, lanes] = (gate[...] * outer).astype(jnp.bfloat16).reshape(col_count, rows, SECOND)

    first_count, second_count = inner.shape[1] // FIRST, width // SECOND

    def grouped(phase):
        return lax.rem(phase - 1 + LEAD, rep_count)

    def phase_step(phase, carry):
        now = grouped(phase)
        last = grouped(phase - 1 + rep_count)
        before = grouped(phase - 2 + rep_count)
        coming = phase + LEAD

        def when(condition, *calls):
            @pl.when(condition)
            def _():
                for call in calls:
                    call()

        first(now, 0)
        weigh(now)
        when(phase > 1, lambda: take_core(last))
        when(coming < rep_count, lambda: take_spread(0, coming))
        for chunk in range(1, first_count):
            first(now, chunk)
        when(coming + 1 < rep_count, lambda: take_rep(coming + 1))
        for chunk in range(second_count):
            second(now, chunk)
            if chunk == second_count // 4:
                when(phase > 2, lambda: take_reduce(stages - 1, before))
            if chunk == second_count // 2:
                for stage in range(1, stages):
                    when(coming < rep_count, functools.partial(take_spread, stage, coming))
                for stage in range(stages - 1):
                    when(phase > 1, functools.partial(take_reduce, stage, last))
        for mask in masks:
            copy_of(("reduce", "core", 0, mask), now).start()
        when(coming < rep_count, lambda: take_all(coming))
        return carry

    lax.fori_loop(1, rep_count + 1, phase_step, 0)
    take_core(grouped(rep_count))
    take_reduce(stages - 1, grouped(rep_count - 1))
    for stage in range(stages):
        take_reduce(stage, grouped(rep_count))
    for half in range(2):
        total = partly(half, stages, 0, 0)[...].astype(jnp.float32)
        for steps in range(1, rep_count):
            copy_of(("reduce", "rep", half, 0), steps).wait_recv()
            total = total + rep_buf[half * rep_count + steps].astype(jnp.float32)
        out_ref[pl.ds(half * half_rows, half_rows)] = total

    def settle(steps, carry):
        for key in number:
            if key[1] == "rep":
                @pl.when(steps != 0)
                def _():
                    copy_of(key, steps).wait_send()
            else:
                copy_of(key, steps).wait_send()
        return carry

    lax.fori_loop(0, rep_count, settle, 0)


def moe_bytes(rep_count, col_count, rows, packed, width, hidden):
    blocks = rep_count * col_count
    masks = col_count // 2
    halves = rep_count * rows * width
    stages = masks.bit_length() - 1
    reduced = sum(halves * (masks >> stage + 1) for stage in range(stages))
    tokens = blocks * rows * (packed + width) + halves * masks + reduced + halves
    return 2 * (tokens + 2 * width * hidden + col_count * rows * hidden + rows * (packed + 2 * width))


def moe_fused(rows, in_weight, out_weight, rep_count, col_count, collective_id):
    bit_count = col_count.bit_length() - 1
    _, _, masks, number = moe_keys(bit_count)
    blocks = rep_count * col_count
    count, packed = rows.shape
    width, hidden = in_weight.shape[1:]
    half = count // 2
    stage_bufs = [
        pltpu.VMEM((2 * rep_count * len(masks) >> stage + 1, half, width), jnp.bfloat16) for stage in range(bit_count - 1)
    ]
    slots = len(number) * rep_count
    return pl.pallas_call(
        functools.partial(moe_kernel, rep_count, col_count),
        out_shape=jax.ShapeDtypeStruct((count, width), jnp.float32),
        in_specs=[pl.BlockSpec(memory_space=pltpu.VMEM)] + [pl.BlockSpec(memory_space=pl.ANY)] * 2,
        out_specs=pl.BlockSpec(memory_space=pltpu.VMEM),
        scratch_shapes=[
            pltpu.VMEM((blocks, count, packed), jnp.bfloat16),
            pltpu.VMEM((width, hidden), jnp.bfloat16),
            pltpu.VMEM((hidden, width), jnp.bfloat16),
            pltpu.VMEM((col_count * count, hidden), jnp.bfloat16),
            pltpu.VMEM((col_count * count, 1), jnp.float32),
            pltpu.VMEM((rep_count, col_count, count, width), jnp.bfloat16),
            pltpu.VMEM((rep_count * len(masks), count, width), jnp.bfloat16),
        ]
        + stage_bufs
        + [
            pltpu.VMEM((2 * rep_count, half, width), jnp.bfloat16),
            pltpu.SemaphoreType.DMA((slots,)),
            pltpu.SemaphoreType.DMA((slots,)),
            pltpu.SemaphoreType.DMA((3,)),
        ],
        compiler_params=pltpu.CompilerParams(
            collective_id=collective_id, has_side_effects=True, vmem_limit_bytes=56 << 20
        ),
    )(rows, in_weight, out_weight)


def served_rows(own_rows, own_sheds, shifts):
    rep_count = lax.axis_size("rep")
    hits = own_sheds[:, None] == jnp.arange(REQ_DEV, dtype=jnp.int32)[None, :]
    leaving = [jnp.sum(jnp.where(hits[k][:, None], own_rows, 0), axis=0, keepdims=True) for k in range(own_sheds.shape[0])]
    leaving = jnp.concatenate(leaving, axis=0)
    arrived = leaving
    for steps in range(1, rep_count):
        moved = shifted(leaving, "rep", steps)
        arrived = jnp.where((shifts == steps)[:, None], moved, arrived)
    served = own_rows
    for k in range(own_sheds.shape[0]):
        served = jnp.where(hits[k][:, None], arrived[k][None, :], served)
    return served


def served_tokens(own_tokens, own_sheds, shifts, collective_id):
    rep_count = lax.axis_size("rep")
    owner = jnp.arange(own_tokens.shape[0], dtype=jnp.int32) // SPEC
    hits = own_sheds[:, None] == owner[None, :]
    width = own_tokens.shape[1]
    blocks = own_tokens.reshape(REQ_DEV, SPEC, width)
    shed = own_sheds.shape[0]
    block_hits = own_sheds[:, None] == jnp.arange(REQ_DEV, dtype=jnp.int32)[None, :]
    leaving = jnp.sum(jnp.where(block_hits[:, :, None, None], blocks[None], 0), axis=1)
    moved = swap(leaving.reshape(shed * SPEC, width), rep_count, collective_id)
    moved = moved.reshape(rep_count - 1, shed, SPEC, width)
    arrived = moved[0]
    for steps in range(2, rep_count):
        arrived = jnp.where((shifts == steps)[:, None, None], moved[steps - 1], arrived)
    served = own_tokens
    for k in range(shed):
        repeated = jnp.tile(arrived[k], (REQ_DEV, 1))
        served = jnp.where(hits[k][:, None], repeated, served)
    return served


def gate_columns(expert_ids, gate_weight, expert_home, device_count):
    target = jnp.sum(
        jnp.where(
            expert_ids[:, :, None] == jnp.arange(device_count, dtype=jnp.int32)[None, None, :],
            expert_home[None, None, :],
            0,
        ),
        axis=2,
    )
    return jnp.sum(
        jnp.where(
            target[:, :, None] == jnp.arange(device_count, dtype=jnp.int32)[None, None, :],
            gate_weight[:, :, None],
            0.0,
        ),
        axis=1,
    )


def moe_split(packed, expert_in, expert_out, me, rep_count, col_count):
    device_count = rep_count * col_count
    everyone = gather_all(packed, rep_count, col_count, 1)
    all_gates = everyone[:, D : D + 2 * device_count].astype(jnp.float32)
    picks = jnp.arange(2 * device_count, dtype=jnp.int32) % device_count == me
    gate = jnp.sum(jnp.where(picks[None, :], all_gates, 0.0), axis=1, keepdims=True)
    inner_act = jax.nn.silu(
        jnp.dot(everyone[:, :D], expert_in[0], preferred_element_type=jnp.float32)
    ).astype(jnp.bfloat16)
    outer_out = jnp.dot(inner_act, expert_out[0], preferred_element_type=jnp.float32)
    return scatter_sum(
        (gate * outer_out).astype(jnp.bfloat16), rep_count, col_count, jnp.float32, 2
    )


def per_device(
    latent_pages,
    queries,
    residual,
    page_count,
    last_fill,
    page_order,
    shed_slots,
    shed_shift,
    expert_ids,
    gate_weight,
    expert_home,
    norm_gain,
    value_up,
    out_weight,
    expert_in,
    expert_out,
):
    rep_count = lax.axis_size("rep")
    col_count = lax.axis_size("ep")
    device_count = rep_count * col_count
    replica = lax.axis_index("rep")
    me = replica * col_count + lax.axis_index("ep")
    own_sheds = shed_slots[replica, 0, :]
    shifts = shed_shift[0]
    served_residual = served_rows(residual, own_sheds, shifts)
    gates = gate_columns(expert_ids, gate_weight, expert_home, device_count)
    gates_high = gates.astype(jnp.bfloat16)
    gates_low = (gates - gates_high.astype(jnp.float32)).astype(jnp.bfloat16)

    tokens_dev = REQ_DEV * SPEC
    heads_dev = value_up.shape[0]
    regrouped = attend(latent_pages, queries, page_count, last_fill, page_order, col_count, 3)
    row_block = regrouped.reshape(tokens_dev * col_count, heads_dev, LAT)
    lifted = jnp.einsum(
        "thl,hlv->thv", row_block, value_up, preferred_element_type=jnp.float32
    ).astype(jnp.bfloat16)
    own_branch = scatter_sum(
        jnp.dot(
            lifted.reshape(tokens_dev * col_count, heads_dev * VHEAD),
            out_weight,
            preferred_element_type=jnp.float32,
        ).astype(jnp.bfloat16),
        1,
        col_count,
        jnp.bfloat16,
        0,
    )
    served_branch = served_tokens(own_branch, own_sheds, shifts, 4)
    attn_proj = served_branch.reshape(REQ_DEV, SPEC * D)
    branch = served_branch.astype(jnp.float32)
    mixed = served_residual.reshape(tokens_dev, D).astype(jnp.float32) + branch
    square = jnp.mean(mixed * mixed, axis=1, keepdims=True)
    normed = (mixed * lax.rsqrt(square + NORM_EPS) * norm_gain).astype(jnp.bfloat16)
    spare = -2 * device_count % 128
    packed = jnp.concatenate(
        (normed, gates_high, gates_low, jnp.zeros((tokens_dev, spare), jnp.bfloat16)), axis=1
    )
    needed = moe_bytes(rep_count, col_count, tokens_dev, packed.shape[1], D, expert_in.shape[2])
    if needed < 52 << 20:
        moe_sum = moe_fused(packed, expert_in, expert_out, rep_count, col_count, 1)
    else:
        moe_sum = moe_split(packed, expert_in, expert_out, me, rep_count, col_count)
    layer_out = (mixed + moe_sum).astype(jnp.bfloat16).reshape(REQ_DEV, SPEC * D)
    return (attn_proj, layer_out)


def solution(mesh):
    placed = (
        P(("rep", "ep"), None),
        P(("rep", "ep"), None),
        P(("rep", "ep"), None),
        P(None, "ep", None),
        P(None, "ep", None),
        P(("rep", "ep"), None),
        P(None, "ep", None),
        P("ep", None),
        P(("rep", "ep"), None),
        P(("rep", "ep"), None),
        P(),
        P(),
        P("ep", None, None),
        P("ep", None),
        P(("rep", "ep"), None, None),
        P(("rep", "ep"), None, None),
    )
    return jax.shard_map(
        per_device,
        mesh=mesh,
        in_specs=placed,
        out_specs=(P(("rep", "ep"), None), P(("rep", "ep"), None)),
        check_vma=False,
    )
```
